32 devices in a mesh: gx: 4 (over x, core), gy: 4 (over z), gz: 2 (over y).
Axes of the slice: x: 2, y: 2, z: 4, core: 2. Of those that a mesh axis runs over, the one named last changes fastest.
Arguments:
- right_side: float32 [16, 16, 8, 4, 256], P('gx', 'gy', 'gz'), may hold values from -80 to 80
- bond_blocks: float32 [13, 4, 4, 16, 16, 8], P(None, None, None, 'gx', 'gy', 'gz'), may hold values from -0.012 to 0.012
- bond_open: int32 [13, 16, 16, 8], P(None, 'gx', 'gy', 'gz'), may hold values 0 or 1
- onsite_blocks: float32 [4, 4, 16, 16, 8], P(None, None, 'gx', 'gy', 'gz'), may hold values from -0.012 to 0.012
- orbital_levels: float32 [4, 16, 16, 8], P(None, 'gx', 'gy', 'gz'), may hold values from 1.3 to 2.6
- column_shift: float32 [256], replicated, may hold values from 0.05 to 1
Outputs:
- solution: float32 [16, 16, 8, 4, 256], P('gx', 'gy', 'gz')
- residual: float32 [16, 16, 8, 4, 256], P('gx', 'gy', 'gz')
The draws below stay inside these ranges and needn't reach their ends.
All inputs are finite; a program needn't handle non-finite values. No bound on the sum of `bond_open` on one device may be relied on, other than what follows from the above.
Results may differ from the reference program's by a relative error of at most 0.0003.
Values sent between devices are 32-bit elements; how exact they have to be, the bound alone decides.
No kernel may reach another device: no remote copies, remote signals or barrier semaphores. Data moves between devices by JAX's collectives and lax.ppermute only.
A program may use at most 192 MiB of HBM per device.

```python
import math
import jax
import jax.numpy as jnp
from jax import lax

ORB = 4
COLS = 256
BONDS = 13
ITERS = 3
NX = 16
NY = 16
NZ = 8


def draw_right_side(key, part):
    subkeys = jax.random.split(key, 3)
    full_shape = (NX, NY, NZ, ORB, COLS)
    along_x = jnp.arange(NX, dtype=jnp.float32) / NX
    along_y = jnp.arange(NY, dtype=jnp.float32) / NY
    along_z = jnp.arange(NZ, dtype=jnp.float32) / NZ
    position_ramp = jnp.exp(0.37 * (along_x[:, None, None] + along_y[None, :, None] + along_z[None, None, :]))
    atom_scale = jnp.exp(jax.random.uniform(subkeys[1], (NX, NY, NZ, ORB, 1), jnp.float32, math.log(0.3), math.log(3.0)))
    values = jnp.clip(jax.random.normal(subkeys[0], full_shape, jnp.float32), -4.0, 4.0)
    column_scale = jnp.exp(jax.random.uniform(subkeys[2], (COLS,), jnp.float32, math.log(0.5), math.log(5.0)))
    return (0.3 * values * atom_scale * column_scale * position_ramp[:, :, :, None, None]).astype(jnp.float32)


def set_ends(array, rng, least, largest):
    shape = array.shape
    place = [jax.random.randint(jax.random.fold_in(rng, axis), (), 0, shape[axis]) for axis in range(len(shape))]
    array = array.at[tuple(place)].set(least)
    longest = shape.index(max(shape))
    place[longest] = (place[longest] + 1) % shape[longest]
    return array.at[tuple(place)].set(largest)


def level_of(key, extent, pieces, smallest, high):
    factor_of, own = 1.0, jax.random.fold_in(key, 6)
    for axis_at, shards_of in pieces:
        steps = jnp.exp(jax.random.uniform(jax.random.fold_in(own, axis_at), (shards_of,), jnp.float32, smallest / len(pieces), high / len(pieces)))
        factor_of = factor_of * jnp.repeat(steps, extent[axis_at] // shards_of).reshape([-1 if axis == axis_at else 1 for axis in range(len(extent))])
    return factor_of


def setup_inputs(seed: int = 0) -> dict:
    keys = jax.random.split(jax.random.key(seed), 7)
    return {
        "right_side": draw_right_side(jax.random.fold_in(keys[6], 71), 0),
        "bond_blocks": jnp.clip(jax.random.uniform(keys[1], (BONDS, ORB, ORB, NX, NY, NZ), jnp.float32, -0.012, 0.012) * level_of(keys[1], (BONDS, ORB, ORB, NX, NY, NZ), ((3, 4), (4, 4), (5, 2)), -0.4, 0.0), -0.012, 0.012),
        "bond_open": set_ends((jax.random.randint(keys[2], (BONDS, NX, NY, NZ), 0, 4) < 3).astype(jnp.int32), jax.random.fold_in(keys[2], 1), 0, 1),
        "onsite_blocks": jnp.clip(jax.random.uniform(keys[3], (ORB, ORB, NX, NY, NZ), jnp.float32, -0.012, 0.012) * level_of(keys[3], (ORB, ORB, NX, NY, NZ), ((2, 4), (3, 4), (4, 2)), -0.4, 0.0), -0.012, 0.012),
        "orbital_levels": jnp.clip(jnp.exp(math.log(2.6) - 0.6931472 * jax.random.uniform(keys[4], (ORB, NX, NY, NZ), jnp.float32) ** level_of(keys[4], (ORB, NX, NY, NZ), ((1, 4), (2, 4), (3, 2)), -0.2, 0.2)), 1.3, 2.6),
        "column_shift": jnp.clip(jnp.exp(jax.random.uniform(keys[5], (COLS,), jnp.float32, math.log(0.05), math.log(1.0))), 0.05, 1.0),
    }


half_offsets = [(first, second, third) for first in (-1, 0, 1) for second in (-1, 0, 1) for third in (-1, 0, 1) if (first, second, third) > (0, 0, 0)]


def hop(blocks, vector):
    return jnp.einsum('ijxyz,xyzjc->xyzic', blocks.astype(jnp.float32), vector.astype(jnp.float32), precision=lax.Precision.HIGHEST)


def operate(vector, coupled, onsite_sym, atom_levels, column_shift):
    result = hop(onsite_sym, vector) + (atom_levels[..., None] + column_shift) * vector
    for bond_index, offset in enumerate(half_offsets):
        ahead = jnp.roll(vector, (-offset[0], -offset[1], -offset[2]), axis=(0, 1, 2))
        behind = jnp.roll(vector, offset, axis=(0, 1, 2))
        mirrored = jnp.roll(coupled[bond_index], offset, axis=(2, 3, 4))
        result = result + hop(coupled[bond_index], ahead) + hop(jnp.swapaxes(mirrored, 0, 1), behind)
    return result


def reference(right_side, bond_blocks, bond_open, onsite_blocks, orbital_levels, column_shift):
    coupled = bond_blocks * bond_open[:, None, None].astype(jnp.float32)
    onsite_sym = 0.5 * (onsite_blocks + jnp.swapaxes(onsite_blocks, 0, 1))
    atom_levels = jnp.transpose(orbital_levels, (1, 2, 3, 0))
    solution = jnp.zeros_like(right_side)
    residual = right_side
    direction = right_side
    norm_now = jnp.sum(residual * residual, axis=(0, 1, 2, 3))
    for iteration in range(ITERS):
        image = operate(direction, coupled, onsite_sym, atom_levels, column_shift)
        alpha = norm_now / jnp.sum(direction * image, axis=(0, 1, 2, 3))
        solution = solution + alpha * direction
        residual = residual - alpha * image
        norm_next = jnp.sum(residual * residual, axis=(0, 1, 2, 3))
        direction = residual + (norm_next / norm_now) * direction
        norm_now = norm_next
    return (solution, residual)
```

```python
import functools

import jax
import jax.numpy as jnp
from jax import lax
from jax.experimental import pallas as pl
from jax.experimental.pallas import tpu as pltpu
from jax.sharding import PartitionSpec as P

ITERS = 3
LANES = 128
ROWS = 16
ALL = ("gx", "gy", "gz")

half_offsets = [
    (first, second, third)
    for first in (-1, 0, 1)
    for second in (-1, 0, 1)
    for third in (-1, 0, 1)
    if (first, second, third) > (0, 0, 0)
]
ONSITE = len(half_offsets)


def shifted(value, axis, by):
    peers = lax.axis_size(axis)
    return lax.ppermute(value, axis, [(i, (i + by) % peers) for i in range(peers)])


def chip_shifted(value, by):
    peers = lax.axis_size("gx")
    return lax.ppermute(value, "gx", [(i, (i + 2 * by) % peers) for i in range(peers)])


def core_swapped(value):
    peers = lax.axis_size("gx")
    return lax.ppermute(value, "gx", [(i, i ^ 1) for i in range(peers)])


def gather_blocks(block):
    count_y, count_z, chips = lax.axis_size("gy"), lax.axis_size("gz"), lax.axis_size("gx") // 2
    along_y = [block] + [shifted(block, "gy", by) for by in range(1, count_y)]
    first = jnp.stack(along_y[: count_y // 2])
    second = jnp.stack(along_y[count_y // 2 :])
    first = jnp.stack([first] + [chip_shifted(first, by) for by in range(1, chips)])
    second = jnp.stack([second] + [shifted(second, "gz", by) for by in range(1, count_z)])
    first = jnp.stack([first] + [shifted(first, "gz", by) for by in range(1, count_z)])
    second = jnp.stack([second] + [chip_shifted(second, by) for by in range(1, chips)])
    own = jnp.concatenate([first.reshape((-1,) + block.shape), second.reshape((-1,) + block.shape)])
    return own, core_swapped(own)


def turn_groups(parts, group, seg):
    count = len(parts)
    bit = 1
    while bit < count:
        high = (group & bit) != 0
        turned = []
        for index in range(count):
            other = parts[index ^ bit]
            if index & bit:
                turned.append(jnp.where(high, parts[index], pltpu.roll(other, LANES - bit * seg, 1)))
            else:
                turned.append(jnp.where(high, pltpu.roll(other, bit * seg, 1), parts[index]))
        parts = turned
        bit *= 2
    return parts


def cg_kernel(sizes, columns_ref, own_ref, other_ref, shift_ref, out_ref, coef, field, image, answer, residual, ahead):
    count_x, count_y, count_z, lx, ly, lz, orbitals = sizes
    seg = lx * lz
    per = LANES // seg
    width = count_x * count_z * seg
    high = count_y * ly
    chips = count_x // 2
    tiles = width // LANES
    halves = ly * orbitals // per
    group = lax.broadcasted_iota(jnp.int32, (1, LANES), 1) // seg
    lane = lax.broadcasted_iota(jnp.int32, (1, width), 1)
    at_z, at_x, at_gz = lane % lz, (lane // lz) % lx, (lane // seg) % count_z
    step_x = seg * count_z - (lx - 1) * lz
    step_z = seg - lz + 1
    wrap_z = (count_z - 1) * seg + lz - 1

    def roll(value, by):
        return pltpu.roll(value, by % width, 1)

    def from_next_z(value):
        return jnp.where(at_z < lz - 1, roll(value, -1), jnp.where(at_gz < count_z - 1, roll(value, -step_z), roll(value, wrap_z)))

    def from_last_z(value):
        return jnp.where(at_z > 0, roll(value, 1), jnp.where(at_gz > 0, roll(value, step_z), roll(value, -wrap_z)))

    def from_next_x(value):
        return jnp.where(at_x < lx - 1, roll(value, -lz), roll(value, -step_x))

    def from_last_x(value):
        return jnp.where(at_x > 0, roll(value, lz), roll(value, step_x))

    def device_of(source, gy):
        return ((source // count_z) * count_y + gy) * count_z + source % count_z

    for gy in range(count_y):
        for tile in range(tiles):
            for half in range(halves):
                parts = [
                    columns_ref[device_of(tile * per + p, gy), :, half * LANES : (half + 1) * LANES]
                    for p in range(per)
                ]
                for g, value in enumerate(turn_groups(parts, group, seg)):
                    y, orb = divmod(half * per + g, orbitals)
                    field[gy * ly + y, orb, :, tile * LANES : (tile + 1) * LANES] = value

    my_x, my_y, my_z = lax.axis_index("gx"), lax.axis_index("gy"), lax.axis_index("gz")
    my_chip, my_core = my_x // 2, my_x % 2
    half_y = count_y // 2

    def fill(gy, carry):
        away = lax.rem(my_y - gy + count_y, count_y)
        near = away < half_y
        for tile in range(tiles):
            slots, cores = [], []
            for p in range(per):
                gx, gz = divmod(tile * per + p, count_z)
                across = lax.rem(my_chip - gx // 2 + chips, chips)
                up = lax.rem(my_z - gz + count_z, count_z)
                slots.append(
                    jnp.where(
                        near,
                        (up * chips + across) * half_y + away,
                        (chips * count_z + across * count_z + up) * half_y + away - half_y,
                    )
                )
                cores.append(gx % 2 == my_core)
            for part in range(orbitals * orbitals * ly // per):
                lanes = slice(part * LANES, (part + 1) * LANES)
                parts = [
                    jnp.where(core, own_ref[slot, :, lanes], other_ref[slot, :, lanes])
                    for slot, core in zip(slots, cores)
                ]
                for g, value in enumerate(turn_groups(parts, group, seg)):
                    pair, y = divmod(part * per + g, ly)
                    coef[gy * ly + y, pair, :, tile * LANES : (tile + 1) * LANES] = value
        return carry

    lax.fori_loop(0, count_y, fill, 0)

    shift = shift_ref[...]
    zero = jnp.zeros(field.shape[2:], jnp.float32)

    def start(y, total):
        for orb in range(orbitals):
            value = field[y, orb]
            residual[y, orb] = value
            total = total + value * value
        return total

    norm_now = jnp.sum(lax.fori_loop(0, high, start, zero), axis=1, keepdims=True)

    directions = ((0, 1), (0, -1), (1, 0), (1, 1), (1, -1))

    def spread(y, carry):
        for orb in range(orbitals):
            value = field[y, orb]
            above, below = from_next_z(value), from_last_z(value)
            ahead[0, y, orb] = above
            ahead[1, y, orb] = below
            ahead[2, y, orb] = from_next_x(value)
            ahead[3, y, orb] = from_next_x(above)
            ahead[4, y, orb] = from_next_x(below)
        return carry

    def apply(y, total):
        rows = {0: y, 1: lax.rem(y + 1, high), -1: lax.rem(y + high - 1, high)}

        def factor(row, i, j, k):
            return coef[row, i * orbitals + j, k : k + 1, :]

        here = [field[y, orb] for orb in range(orbitals)]
        result = [shift * value for value in here]
        for j in range(orbitals):
            for i in range(orbitals):
                result[i] = result[i] + factor(y, i, j, ONSITE) * here[j]
        for k, (first, second, third) in enumerate(half_offsets):
            for j in range(orbitals):
                if (first, third) == (0, 0):
                    value = field[rows[second], j]
                else:
                    value = ahead[directions.index((first, third)), rows[second], j]
                for i in range(orbitals):
                    result[i] = result[i] + factor(y, i, j, k) * value
        landing = {}
        for first, third in ((0, 0), (0, 1), (0, -1), (1, 0), (1, 1), (1, -1)):
            sums = [None] * orbitals
            for k, offset in enumerate(half_offsets):
                if (offset[0], offset[2]) != (first, third):
                    continue
                row = rows[-offset[1]]
                for j in range(orbitals):
                    value = field[row, j]
                    for i in range(orbitals):
                        term = factor(row, j, i, k) * value
                        sums[i] = term if sums[i] is None else sums[i] + term
            if third == 1:
                sums = [from_last_z(value) for value in sums]
            elif third == -1:
                sums = [from_next_z(value) for value in sums]
            landing[first] = [a + b for a, b in zip(landing[first], sums)] if first in landing else sums
        for i in range(orbitals):
            value = result[i] + landing[0][i] + from_last_x(landing[1][i])
            image[y, i] = value
            total = total + value * here[i]
        return total

    for iteration in range(ITERS):
        lax.fori_loop(0, high, spread, 0)
        product = jnp.sum(lax.fori_loop(0, high, apply, zero), axis=1, keepdims=True)
        alpha = norm_now / product

        def advance(y, total):
            for orb in range(orbitals):
                move = alpha * field[y, orb]
                answer[y, orb] = move if iteration == 0 else answer[y, orb] + move
                value = residual[y, orb] - alpha * image[y, orb]
                residual[y, orb] = value
                total = total + value * value
            return total

        total = lax.fori_loop(0, high, advance, zero)
        if iteration + 1 < ITERS:
            norm_next = jnp.sum(total, axis=1, keepdims=True)
            ratio = norm_next / norm_now

            def turn(y, carry):
                for orb in range(orbitals):
                    field[y, orb] = residual[y, orb] + ratio * field[y, orb]
                return carry

            lax.fori_loop(0, high, turn, 0)
            norm_now = norm_next

    for which, source in enumerate((answer, residual)):
        for gy in range(count_y):
            for tile in range(tiles):
                for half in range(halves):
                    parts = []
                    for g in range(per):
                        y, orb = divmod(half * per + g, orbitals)
                        parts.append(source[gy * ly + y, orb, :, tile * LANES : (tile + 1) * LANES])
                    for p, value in enumerate(turn_groups(parts, group, seg)):
                        out_ref[device_of(tile * per + p, gy), which, :, half * LANES : (half + 1) * LANES] = value


def block_kernel(bonds_ref, open_ref, onsite_ref, levels_ref, out_ref, rows):
    orbitals, lx, ly, lz = levels_ref.shape
    bonds = bonds_ref.shape[-1]
    rows[...] = jnp.zeros_like(rows)
    eye = (
        lax.broadcasted_iota(jnp.int32, (lz, lz), 0) == lax.broadcasted_iota(jnp.int32, (lz, lz), 1)
    ).astype(jnp.float32)
    for i in range(orbitals):
        for j in range(orbitals):
            for x in range(lx):
                local = 0.5 * (onsite_ref[i, j, x] + onsite_ref[j, i, x])
                if i == j:
                    local = local + levels_ref[i, x]
                for y in range(ly):
                    row = (((i * orbitals + j) * ly + y) * lx + x) * lz
                    mask = open_ref[x * ly + y].astype(jnp.float32)
                    rows[row : row + lz, :bonds] = bonds_ref[((i * orbitals + j) * lx + x) * ly + y] * mask
                    rows[row : row + lz, bonds : bonds + lz] = eye * local[y : y + 1, :]
    turned = jnp.transpose(rows[...])
    last = jnp.sum(turned[bonds : bonds + lz], axis=0, keepdims=True)
    place = lax.broadcasted_iota(jnp.int32, out_ref.shape, 0)
    out_ref[...] = jnp.where(place < bonds, turned[:ROWS], jnp.where(place == bonds, last, 0.0))


def pack_kernel(field_ref, out_ref, rows):
    lx, ly, lz, orbitals, _ = field_ref.shape
    for x in range(lx):
        for y in range(ly):
            for z in range(lz):
                base = y * orbitals * lx * lz + x * lz + z
                for tile in range(rows.shape[0]):
                    lanes = slice(tile * LANES, (tile + 1) * LANES)
                    rows[tile, pl.ds(base, orbitals, stride=lx * lz), :] = field_ref[x, y, z, :, lanes]
    for tile in range(rows.shape[0]):
        out_ref[tile * LANES : (tile + 1) * LANES, :] = jnp.transpose(rows[tile])


def unpack_kernel(back_ref, answer_ref, residual_ref, rows):
    lx, ly, lz, orbitals, columns = answer_ref.shape
    for which, out_ref in enumerate((answer_ref, residual_ref)):
        turned = jnp.transpose(back_ref[:, which].reshape(columns, -1))
        for tile in range(rows.shape[1]):
            rows[which, tile] = turned[:, tile * LANES : (tile + 1) * LANES]
        for x in range(lx):
            for y in range(ly):
                for z in range(lz):
                    base = y * orbitals * lx * lz + x * lz + z
                    for tile in range(rows.shape[1]):
                        lanes = slice(tile * LANES, (tile + 1) * LANES)
                        out_ref[x, y, z, :, lanes] = rows[which, tile, pl.ds(base, orbitals, stride=lx * lz), :]


def per_device(right_side, bond_blocks, bond_open, onsite_blocks, orbital_levels, column_shift):
    lx, ly, lz, orbitals, columns = right_side.shape
    count_x, count_y, count_z = (lax.axis_size(axis) for axis in ALL)
    devices = count_x * count_y * count_z
    own_columns = columns // devices
    padded = -(-own_columns // 8) * 8
    seg = lx * lz
    width = count_x * count_z * seg
    high = count_y * ly
    assert LANES % seg == 0 and width % LANES == 0 and count_x % 2 == 0 and count_y % 2 == 0
    assert (ly * orbitals) % (LANES // seg) == 0 and columns % devices == 0

    atoms = lx * ly * lz
    bonds = bond_blocks.shape[0]
    vmem = pl.BlockSpec(memory_space=pltpu.VMEM)
    block = pl.pallas_call(
        block_kernel,
        out_shape=jax.ShapeDtypeStruct((ROWS, orbitals * orbitals * atoms), jnp.float32),
        in_specs=[vmem] * 4,
        out_specs=vmem,
        scratch_shapes=[pltpu.VMEM((orbitals * orbitals * atoms, LANES), jnp.float32)],
        name="block",
    )(
        jnp.transpose(bond_blocks, (1, 2, 3, 4, 5, 0)).reshape(-1, lz, bonds),
        jnp.transpose(bond_open, (1, 2, 3, 0)).reshape(-1, lz, bonds),
        onsite_blocks,
        orbital_levels,
    )
    own, other = gather_blocks(block)

    packed = pl.pallas_call(
        pack_kernel,
        out_shape=jax.ShapeDtypeStruct((columns, orbitals * atoms), jnp.float32),
        in_specs=[vmem],
        out_specs=vmem,
        scratch_shapes=[pltpu.VMEM((columns // LANES, orbitals * atoms, LANES), jnp.float32)],
        name="pack",
    )(right_side)
    packed = packed.reshape(devices, own_columns, orbitals * atoms)
    received = lax.all_to_all(packed, ALL, 0, 0, tiled=True)
    index = (lax.axis_index("gx") * count_y + lax.axis_index("gy")) * count_z + lax.axis_index("gz")
    shift = lax.dynamic_slice_in_dim(column_shift, index * own_columns, own_columns)
    if padded != own_columns:
        received = jnp.pad(received, ((0, 0), (0, padded - own_columns), (0, 0)))
        shift = jnp.pad(shift, (0, padded - own_columns))
    shift = jnp.broadcast_to(shift[:, None], (padded, width))

    sizes = (count_x, count_y, count_z, lx, ly, lz, orbitals)
    state = pltpu.VMEM((high, orbitals, padded, width), jnp.float32)
    out = pl.pallas_call(
        functools.partial(cg_kernel, sizes),
        out_shape=jax.ShapeDtypeStruct((devices, 2, padded, ly * orbitals * seg), jnp.float32),
        in_specs=[pl.BlockSpec(memory_space=pltpu.VMEM)] * 4,
        out_specs=pl.BlockSpec(memory_space=pltpu.VMEM),
        scratch_shapes=[
            pltpu.VMEM((high, orbitals * orbitals, ROWS, width), jnp.float32),
            state,
            state,
            state,
            state,
            pltpu.VMEM((5, high, orbitals, padded, width), jnp.float32),
        ],
        compiler_params=pltpu.CompilerParams(vmem_limit_bytes=56 * 1024 * 1024),
        name="cg",
    )(received, own, other, shift)
    if padded != own_columns:
        out = out[:, :, :own_columns]
    back = lax.all_to_all(out, ALL, 0, 0, tiled=True)
    shape = jax.ShapeDtypeStruct(right_side.shape, jnp.float32)
    return tuple(
        pl.pallas_call(
            unpack_kernel,
            out_shape=(shape, shape),
            in_specs=[vmem],
            out_specs=(vmem, vmem),
            scratch_shapes=[pltpu.VMEM((2, columns // LANES, orbitals * atoms, LANES), jnp.float32)],
            name="unpack",
        )(back)
    )


def solution(mesh):
    placed = (
        P("gx", "gy", "gz", None, None),
        P(None, None, None, "gx", "gy", "gz"),
        P(None, "gx", "gy", "gz"),
        P(None, None, "gx", "gy", "gz"),
        P(None, "gx", "gy", "gz"),
        P(),
    )
    return jax.shard_map(
        per_device,
        mesh=mesh,
        in_specs=placed,
        out_specs=(P("gx", "gy", "gz", None, None), P("gx", "gy", "gz", None, None)),
        check_vma=False,
    )
```

```python
import functools

import jax
import jax.numpy as jnp
import numpy as np
from jax import lax
from jax.experimental import pallas as pl
from jax.experimental.pallas import tpu as pltpu
from jax.sharding import PartitionSpec as P


ITERS = 3
LANES = 128
ROWS = 16
PARTS = 8
ALL = ("gx", "gy", "gz")

half_offsets = [
    (first, second, third)
    for first in (-1, 0, 1)
    for second in (-1, 0, 1)
    for third in (-1, 0, 1)
    if (first, second, third) > (0, 0, 0)
]
ONSITE = len(half_offsets)


def shifted(value, axis, by):
    peers = lax.axis_size(axis)
    return lax.ppermute(value, axis, [(i, (i + by) % peers) for i in range(peers)])


def chip_shifted(value, by):
    peers = lax.axis_size("gx")
    return lax.ppermute(value, "gx", [(i, (i + 2 * by) % peers) for i in range(peers)])


def core_swapped(value):
    peers = lax.axis_size("gx")
    return lax.ppermute(value, "gx", [(i, i ^ 1) for i in range(peers)])


def gather_blocks(block):
    count_y, count_z, chips = lax.axis_size("gy"), lax.axis_size("gz"), lax.axis_size("gx") // 2
    along_y = [block] + [shifted(block, "gy", by) for by in range(1, count_y)]
    first = jnp.stack(along_y[: count_y // 2])
    second = jnp.stack(along_y[count_y // 2 :])
    first = jnp.stack([first] + [chip_shifted(first, by) for by in range(1, chips)])
    second = jnp.stack([second] + [shifted(second, "gz", by) for by in range(1, count_z)])
    first = jnp.stack([first] + [shifted(first, "gz", by) for by in range(1, count_z)])
    second = jnp.stack([second] + [chip_shifted(second, by) for by in range(1, chips)])
    own = jnp.concatenate([first.reshape((-1,) + block.shape), second.reshape((-1,) + block.shape)])
    return own, core_swapped(own)


def lane_plan(sizes, dx, dz):
    count_x, _, count_z, lx, _, lz, _ = sizes
    width = count_x * count_z * lx * lz
    lane = np.arange(width)
    tile, inner = lane // LANES, lane % LANES
    part = (inner // (4 * lx * lz)) * 4 + (inner // (2 * lx * lz)) % 2 * 2 + (inner // lz) % 2
    source = tile * PARTS + part
    x = source // count_z * lx + (inner // (2 * lz)) % lx
    z = source % count_z * lz + inner % lz
    place = np.zeros((count_x * lx, count_z * lz), np.int64)
    place[x, z] = lane
    wanted = place[(x + dx) % (count_x * lx), (z + dz) % (count_z * lz)]
    by = (lane - wanted) % width
    return [(int(step), by == step) for step in sorted(set(by.tolist()), key=lambda n: -np.sum(by == n))]


def all_plans(sizes):
    return {name: lane_plan(sizes, *name) for name in ((0, 1), (0, -1), (1, 0), (-1, 0))}


def turn_groups(parts, lane, strides):
    bit = len(parts) // 2
    for stride in strides:
        high = (lane // stride) % 2 == 1
        turned = []
        for index in range(len(parts)):
            other = parts[index ^ bit]
            if index & bit:
                turned.append(jnp.where(high, parts[index], pltpu.roll(other, LANES - stride, 1)))
            else:
                turned.append(jnp.where(high, pltpu.roll(other, stride, 1), parts[index]))
        parts = turned
        bit //= 2
    return parts


def cg_kernel(sizes, columns_ref, own_ref, other_ref, shift_ref, mask_ref, out_ref, coef, field, image, answer, residual, ahead):
    count_x, count_y, count_z, lx, ly, lz, orbitals = sizes
    width = count_x * count_z * lx * lz
    high = count_y * ly
    chips = count_x // 2
    tiles = width // LANES
    lane = lax.broadcasted_iota(jnp.int32, (1, LANES), 1)
    strides = (4 * lx * lz, 2 * lx * lz, lz)
    moves, row = {}, 0
    for name, plan in all_plans(sizes).items():
        moves[name] = [(plan[0][0], None)]
        for by, _ in plan[1:]:
            moves[name].append((by, mask_ref[row : row + 1, :] != 0))
            row += 1

    def take(value, name):
        result = None
        for by, mask in moves[name]:
            rolled = pltpu.roll(value, by, 1)
            result = rolled if mask is None else jnp.where(mask, rolled, result)
        return result

    def device_of(source, gy):
        return ((source // count_z) * count_y + gy) * count_z + source % count_z

    for gy in range(count_y):
        for tile in range(tiles):
            for half in range(ly // 2):
                lanes = slice(half * LANES, (half + 1) * LANES)
                parts = [columns_ref[device_of(tile * PARTS + p, gy), :, lanes] for p in range(PARTS)]
                for g, value in enumerate(turn_groups(parts, lane, strides)):
                    field[gy * ly + half * 2 + g % 2, g // 2, :, tile * LANES : (tile + 1) * LANES] = value

    my_x, my_y, my_z = lax.axis_index("gx"), lax.axis_index("gy"), lax.axis_index("gz")
    my_chip, my_core = my_x // 2, my_x % 2
    half_y = count_y // 2

    def fill(gy, carry):
        away = lax.rem(my_y - gy + count_y, count_y)
        near = away < half_y
        for tile in range(tiles):
            slots, cores = [], []
            for p in range(PARTS):
                gx, gz = divmod(tile * PARTS + p, count_z)
                across = lax.rem(my_chip - gx // 2 + chips, chips)
                up = lax.rem(my_z - gz + count_z, count_z)
                slots.append(
                    jnp.where(
                        near,
                        (up * chips + across) * half_y + away,
                        (chips * count_z + across * count_z + up) * half_y + away - half_y,
                    )
                )
                cores.append(gx % 2 == my_core)
            for part in range(orbitals * orbitals // 2):
                lanes = slice(part * LANES, (part + 1) * LANES)
                parts = [
                    jnp.where(core, own_ref[slot, :, lanes], other_ref[slot, :, lanes])
                    for slot, core in zip(slots, cores)
                ]
                for g, value in enumerate(turn_groups(parts, lane, strides)):
                    coef[gy * ly + g % ly, part * 2 + g // ly, :, tile * LANES : (tile + 1) * LANES] = value
        return carry

    lax.fori_loop(0, count_y, fill, 0)

    shift = shift_ref[...]
    zero = jnp.zeros(field.shape[2:], jnp.float32)

    def start(y, total):
        for orb in range(orbitals):
            value = field[y, orb]
            residual[y, orb] = value
            total = total + value * value
        return total

    norm_now = jnp.sum(lax.fori_loop(0, high, start, zero), axis=1, keepdims=True)

    directions = ((0, 1), (0, -1), (1, 0), (1, 1), (1, -1))

    def spread(y):
        rows = []
        for orb in range(orbitals):
            value = field[y, orb]
            above, below = take(value, (0, 1)), take(value, (0, -1))
            rows.append((above, below, take(value, (1, 0)), take(above, (1, 0)), take(below, (1, 0))))
        return rows

    def keep(y, rows):
        for orb, values in enumerate(rows):
            for which, value in enumerate(values):
                ahead[which, y, orb] = value

    def apply(y, total):
        rows = {0: y, 1: lax.rem(y + 1, high), -1: lax.rem(y + high - 1, high)}
        coming = lax.rem(y + 2, high)
        spread_rows = spread(coming)

        def factor(row, i, j, k):
            return coef[row, i * orbitals + j, k : k + 1, :]

        here = [field[y, orb] for orb in range(orbitals)]
        result = [shift * value for value in here]
        for j in range(orbitals):
            for i in range(orbitals):
                result[i] = result[i] + factor(y, i, j, ONSITE) * here[j]
        for k, (first, second, third) in enumerate(half_offsets):
            for j in range(orbitals):
                if (first, third) == (0, 0):
                    value = field[rows[second], j]
                else:
                    value = ahead[directions.index((first, third)), rows[second], j]
                for i in range(orbitals):
                    result[i] = result[i] + factor(y, i, j, k) * value
        landing = {}
        for first, third in ((0, 0), (0, 1), (0, -1), (1, 0), (1, 1), (1, -1)):
            sums = [None] * orbitals
            for k, offset in enumerate(half_offsets):
                if (offset[0], offset[2]) != (first, third):
                    continue
                row = rows[-offset[1]]
                for j in range(orbitals):
                    value = field[row, j]
                    for i in range(orbitals):
                        term = factor(row, j, i, k) * value
                        sums[i] = term if sums[i] is None else sums[i] + term
            if third == 1:
                sums = [take(value, (0, -1)) for value in sums]
            elif third == -1:
                sums = [take(value, (0, 1)) for value in sums]
            landing[first] = [a + b for a, b in zip(landing[first], sums)] if first in landing else sums
        for i in range(orbitals):
            value = result[i] + landing[0][i] + take(landing[1][i], (-1, 0))
            image[y, i] = value
            total = total + value * here[i]
        keep(coming, spread_rows)
        return total

    for iteration in range(ITERS):
        for y in (high - 1, 0, 1):
            keep(y, spread(y))
        product = jnp.sum(lax.fori_loop(0, high, apply, zero), axis=1, keepdims=True)
        alpha = norm_now / product

        def advance(y, total):
            for orb in range(orbitals):
                move = alpha * field[y, orb]
                answer[y, orb] = move if iteration == 0 else answer[y, orb] + move
                value = residual[y, orb] - alpha * image[y, orb]
                residual[y, orb] = value
                total = total + value * value
            return total

        total = lax.fori_loop(0, high, advance, zero)
        if iteration + 1 < ITERS:
            norm_next = jnp.sum(total, axis=1, keepdims=True)
            ratio = norm_next / norm_now

            def turn(y, carry):
                for orb in range(orbitals):
                    field[y, orb] = residual[y, orb] + ratio * field[y, orb]
                return carry

            lax.fori_loop(0, high, turn, 0)
            norm_now = norm_next

    for which, source in enumerate((answer, residual)):
        for gy in range(count_y):
            for tile in range(tiles):
                for half in range(ly // 2):
                    lanes = slice(tile * LANES, (tile + 1) * LANES)
                    parts = [source[gy * ly + half * 2 + g % 2, g // 2, :, lanes] for g in range(PARTS)]
                    for p, value in enumerate(turn_groups(parts, lane, strides)):
                        out_ref[device_of(tile * PARTS + p, gy), which, :, half * LANES : (half + 1) * LANES] = value


def block_kernel(bonds_ref, open_ref, onsite_ref, levels_ref, out_ref, rows):
    orbitals, lx, ly, lz = levels_ref.shape
    bonds = bonds_ref.shape[-1]
    rows[...] = jnp.zeros_like(rows)
    eye = (
        lax.broadcasted_iota(jnp.int32, (lz, lz), 0) == lax.broadcasted_iota(jnp.int32, (lz, lz), 1)
    ).astype(jnp.float32)
    for i in range(orbitals):
        for j in range(orbitals):
            for x in range(lx):
                local = 0.5 * (onsite_ref[i, j, x] + onsite_ref[j, i, x])
                if i == j:
                    local = local + levels_ref[i, x]
                for y in range(ly):
                    row = ((((i * orbitals + j) * (ly // 2) + y // 2) * lx + x) * 2 + y % 2) * lz
                    mask = open_ref[x * ly + y].astype(jnp.float32)
                    rows[row : row + lz, :bonds] = bonds_ref[((i * orbitals + j) * lx + x) * ly + y] * mask
                    rows[row : row + lz, bonds : bonds + lz] = eye * local[y : y + 1, :]
    turned = jnp.transpose(rows[...])
    last = jnp.sum(turned[bonds : bonds + lz], axis=0, keepdims=True)
    place = lax.broadcasted_iota(jnp.int32, out_ref.shape, 0)
    out_ref[...] = jnp.where(place < bonds, turned[:ROWS], jnp.where(place == bonds, last, 0.0))


def pack_kernel(field_ref, out_ref, rows):
    lx, ly, lz, orbitals, _ = field_ref.shape
    for x in range(lx):
        for y in range(ly):
            for z in range(lz):
                base = ((y // 2 * orbitals * lx + x) * 2 + y % 2) * lz + z
                for tile in range(rows.shape[0]):
                    lanes = slice(tile * LANES, (tile + 1) * LANES)
                    rows[tile, pl.ds(base, orbitals, stride=2 * lx * lz), :] = field_ref[x, y, z, :, lanes]
    for tile in range(rows.shape[0]):
        out_ref[tile * LANES : (tile + 1) * LANES, :] = jnp.transpose(rows[tile])


def unpack_kernel(back_ref, answer_ref, residual_ref, rows):
    lx, ly, lz, orbitals, columns = answer_ref.shape
    for which, out_ref in enumerate((answer_ref, residual_ref)):
        turned = jnp.transpose(back_ref[:, which].reshape(columns, -1))
        for tile in range(rows.shape[1]):
            rows[which, tile] = turned[:, tile * LANES : (tile + 1) * LANES]
        for x in range(lx):
            for y in range(ly):
                for z in range(lz):
                    base = ((y // 2 * orbitals * lx + x) * 2 + y % 2) * lz + z
                    for tile in range(rows.shape[1]):
                        lanes = slice(tile * LANES, (tile + 1) * LANES)
                        out_ref[x, y, z, :, lanes] = rows[which, tile, pl.ds(base, orbitals, stride=2 * lx * lz), :]


def per_device(right_side, bond_blocks, bond_open, onsite_blocks, orbital_levels, column_shift):
    lx, ly, lz, orbitals, columns = right_side.shape
    count_x, count_y, count_z = (lax.axis_size(axis) for axis in ALL)
    devices = count_x * count_y * count_z
    own_columns = columns // devices
    padded = -(-own_columns // 8) * 8
    width = count_x * count_z * lx * lz
    high = count_y * ly
    assert (lx, ly, lz, orbitals) == (4, 4, 4, 4) and columns % devices == 0
    assert count_x % 2 == 0 and count_y % 2 == 0 and count_x * count_z % PARTS == 0

    atoms = lx * ly * lz
    bonds = bond_blocks.shape[0]
    vmem = pl.BlockSpec(memory_space=pltpu.VMEM)
    block = pl.pallas_call(
        block_kernel,
        out_shape=jax.ShapeDtypeStruct((ROWS, orbitals * orbitals * atoms), jnp.float32),
        in_specs=[vmem] * 4,
        out_specs=vmem,
        scratch_shapes=[pltpu.VMEM((orbitals * orbitals * atoms, LANES), jnp.float32)],
        name="block",
    )(
        jnp.transpose(bond_blocks, (1, 2, 3, 4, 5, 0)).reshape(-1, lz, bonds),
        jnp.transpose(bond_open, (1, 2, 3, 0)).reshape(-1, lz, bonds),
        onsite_blocks,
        orbital_levels,
    )
    own, other = gather_blocks(block)

    packed = pl.pallas_call(
        pack_kernel,
        out_shape=jax.ShapeDtypeStruct((columns, orbitals * atoms), jnp.float32),
        in_specs=[vmem],
        out_specs=vmem,
        scratch_shapes=[pltpu.VMEM((columns // LANES, orbitals * atoms, LANES), jnp.float32)],
        name="pack",
    )(right_side)
    packed = packed.reshape(devices, own_columns, orbitals * atoms)
    received = lax.all_to_all(packed, ALL, 0, 0, tiled=True)
    index = (lax.axis_index("gx") * count_y + lax.axis_index("gy")) * count_z + lax.axis_index("gz")
    shift = lax.dynamic_slice_in_dim(column_shift, index * own_columns, own_columns)
    if padded != own_columns:
        received = jnp.pad(received, ((0, 0), (0, padded - own_columns), (0, 0)))
        shift = jnp.pad(shift, (0, padded - own_columns))
    shift = jnp.broadcast_to(shift[:, None], (padded, width))

    sizes = (count_x, count_y, count_z, lx, ly, lz, orbitals)
    masks = [lanes for plan in all_plans(sizes).values() for _, lanes in plan[1:]]
    masks = jnp.asarray(np.stack(masks).astype(np.int32))
    state = pltpu.VMEM((high, orbitals, padded, width), jnp.float32)
    out = pl.pallas_call(
        functools.partial(cg_kernel, sizes),
        out_shape=jax.ShapeDtypeStruct((devices, 2, padded, orbitals * lx * ly * lz), jnp.float32),
        in_specs=[vmem] * 5,
        out_specs=vmem,
        scratch_shapes=[
            pltpu.VMEM((high, orbitals * orbitals, ROWS, width), jnp.float32),
            state,
            state,
            state,
            state,
            pltpu.VMEM((5, high, orbitals, padded, width), jnp.float32),
        ],
        compiler_params=pltpu.CompilerParams(vmem_limit_bytes=(8 + 24 * width // 512) * 1024 * 1024 * 2),
        name="cg",
    )(received, own, other, shift, masks)
    if padded != own_columns:
        out = out[:, :, :own_columns]
    back = lax.all_to_all(out, ALL, 0, 0, tiled=True)
    shape = jax.ShapeDtypeStruct(right_side.shape, jnp.float32)
    return tuple(
        pl.pallas_call(
            unpack_kernel,
            out_shape=(shape, shape),
            in_specs=[vmem],
            out_specs=(vmem, vmem),
            scratch_shapes=[pltpu.VMEM((2, columns // LANES, orbitals * atoms, LANES), jnp.float32)],
            name="unpack",
        )(back)
    )


def solution(mesh):
    placed = (
        P("gx", "gy", "gz", None, None),
        P(None, None, None, "gx", "gy", "gz"),
        P(None, "gx", "gy", "gz"),
        P(None, None, "gx", "gy", "gz"),
        P(None, "gx", "gy", "gz"),
        P(),
    )
    return jax.shard_map(
        per_device,
        mesh=mesh,
        in_specs=placed,
        out_specs=(P("gx", "gy", "gz", None, None), P("gx", "gy", "gz", None, None)),
        check_vma=False,
    )
```

```python
import functools

import jax
import jax.numpy as jnp
import numpy as np
from jax import lax
from jax.experimental import pallas as pl
from jax.experimental.pallas import tpu as pltpu
from jax.sharding import PartitionSpec as P


ITERS = 3
LANES = 128
PARTS = 8
ALL = ("gx", "gy", "gz")

half_offsets = [
    (first, second, third)
    for first in (-1, 0, 1)
    for second in (-1, 0, 1)
    for third in (-1, 0, 1)
    if (first, second, third) > (0, 0, 0)
]
ONSITE = len(half_offsets)


def shifted(value, axis, by):
    peers = lax.axis_size(axis)
    return lax.ppermute(value, axis, [(i, (i + by) % peers) for i in range(peers)])


def chip_shifted(value, by):
    peers = lax.axis_size("gx")
    return lax.ppermute(value, "gx", [(i, (i + 2 * by) % peers) for i in range(peers)])


def core_swapped(value):
    peers = lax.axis_size("gx")
    return lax.ppermute(value, "gx", [(i, i ^ 1) for i in range(peers)])


def gather_blocks(block):
    count_y, count_z, chips = lax.axis_size("gy"), lax.axis_size("gz"), lax.axis_size("gx") // 2
    along_y = [block] + [shifted(block, "gy", by) for by in range(1, count_y)]
    first = jnp.stack(along_y[: count_y // 2])
    second = jnp.stack(along_y[count_y // 2 :])
    first = jnp.stack([first] + [chip_shifted(first, by) for by in range(1, chips)])
    second = jnp.stack([second] + [shifted(second, "gz", by) for by in range(1, count_z)])
    first = jnp.stack([first] + [shifted(first, "gz", by) for by in range(1, count_z)])
    second = jnp.stack([second] + [chip_shifted(second, by) for by in range(1, chips)])
    own = jnp.concatenate([first.reshape((-1,) + block.shape), second.reshape((-1,) + block.shape)])
    return own, core_swapped(own)


def lane_plan(sizes, dx, dz):
    count_x, _, count_z, lx, _, lz, _ = sizes
    width = count_x * count_z * lx * lz
    lane = np.arange(width)
    tile, inner = lane // LANES, lane % LANES
    part = (inner // (4 * lx * lz)) * 4 + (inner // (2 * lx * lz)) % 2 * 2 + (inner // lz) % 2
    source = tile * PARTS + part
    x = source // count_z * lx + (inner // (2 * lz)) % lx
    z = source % count_z * lz + inner % lz
    place = np.zeros((count_x * lx, count_z * lz), np.int64)
    place[x, z] = lane
    wanted = place[(x + dx) % (count_x * lx), (z + dz) % (count_z * lz)]
    by = (lane - wanted) % width
    return [(int(step), by == step) for step in sorted(set(by.tolist()), key=lambda n: -np.sum(by == n))]


def lanes_from(value, places):
    return jnp.take_along_axis(value, places, axis=1, mode="promise_in_bounds")


def all_plans(sizes):
    return {name: lane_plan(sizes, *name) for name in ((0, 1), (0, -1), (1, 0), (-1, 0))}


def turn_groups(parts, lane, strides):
    bit = len(parts) // 2
    for stride in strides:
        high = (lane // stride) % 2 == 1
        partner = jnp.where(high, lane - stride, lane + stride)
        turned = list(parts)
        for index in range(len(parts)):
            if index & bit == 0:
                low, top = parts[index], parts[index | bit]
                crossing = lanes_from(jnp.where(high, low, top), partner)
                turned[index] = jnp.where(high, crossing, low)
                turned[index | bit] = jnp.where(high, top, crossing)
        parts = turned
        bit //= 2
    return parts


def cg_kernel(sizes, columns_ref, own_ref, other_ref, shift_ref, mask_ref, out_ref, coef, field, image, answer, residual, ahead):
    count_x, count_y, count_z, lx, ly, lz, orbitals = sizes
    width = count_x * count_z * lx * lz
    high = count_y * ly
    chips = count_x // 2
    tiles = width // LANES
    height = columns_ref.shape[1]
    assert height == 8
    lane = lax.broadcasted_iota(jnp.int32, (height, LANES), 1)
    strides = (4 * lx * lz, 2 * lx * lz, lz)
    moves, row = {}, 0
    for name, plan in all_plans(sizes).items():
        if width == LANES and len(plan) > 1:
            places = lane - plan[0][0]
            for by, _ in plan[1:]:
                places = jnp.where(mask_ref[row : row + 1, :] != 0, lane - by, places)
                row += 1
            moves[name] = places & (LANES - 1)
            continue
        moves[name] = [(plan[0][0], None)]
        for by, _ in plan[1:]:
            moves[name].append((by, mask_ref[row : row + 1, :] != 0))
            row += 1

    def take(value, name):
        if not isinstance(moves[name], list):
            return lanes_from(value, moves[name])
        result = None
        for by, mask in moves[name]:
            rolled = pltpu.roll(value, by, 1)
            result = rolled if mask is None else jnp.where(mask, rolled, result)
        return result

    def device_of(source, gy):
        return ((source // count_z) * count_y + gy) * count_z + source % count_z

    for gy in range(count_y):
        for tile in range(tiles):
            for half in range(ly // 2):
                lanes = slice(half * LANES, (half + 1) * LANES)
                parts = [columns_ref[device_of(tile * PARTS + p, gy), :, lanes] for p in range(PARTS)]
                for g, value in enumerate(turn_groups(parts, lane, strides)):
                    field[gy * ly + half * 2 + g % 2, g // 2, :, tile * LANES : (tile + 1) * LANES] = value

    my_x, my_y, my_z = lax.axis_index("gx"), lax.axis_index("gy"), lax.axis_index("gz")
    my_chip, my_core = my_x // 2, my_x % 2
    half_y = count_y // 2

    def fill(gy, carry):
        away = lax.rem(my_y - gy + count_y, count_y)
        near = away < half_y
        for tile in range(tiles):
            slots, cores = [], []
            for p in range(PARTS):
                gx, gz = divmod(tile * PARTS + p, count_z)
                across = lax.rem(my_chip - gx // 2 + chips, chips)
                up = lax.rem(my_z - gz + count_z, count_z)
                slots.append(
                    jnp.where(
                        near,
                        (up * chips + across) * half_y + away,
                        (chips * count_z + across * count_z + up) * half_y + away - half_y,
                    )
                )
                cores.append(gx % 2 == my_core)
            for k in range(ONSITE + 1):
                rows = slice(k * 8, k * 8 + 8)
                parts = [
                    jnp.where(core, own_ref[slot, rows, :], other_ref[slot, rows, :])
                    for slot, core in zip(slots, cores)
                ]
                for g, value in enumerate(turn_groups(parts, lane, strides)):
                    first = g // ly * 8
                    coef[gy * ly + g % ly, k, first : first + 8, tile * LANES : (tile + 1) * LANES] = value
        return carry

    lax.fori_loop(0, count_y, fill, 0)

    shift = shift_ref[...]
    zero = jnp.zeros(field.shape[2:], jnp.float32)

    def start(y, total):
        for orb in range(orbitals):
            value = field[y, orb]
            residual[y, orb] = value
            total = total + value * value
        return total

    norm_now = jnp.sum(lax.fori_loop(0, high, start, zero, unroll=4), axis=1, keepdims=True)

    directions = ((0, 1), (0, -1), (1, 0), (1, 1), (1, -1))

    def spread(y):
        rows = []
        for orb in range(orbitals):
            value = field[y, orb]
            above, below = take(value, (0, 1)), take(value, (0, -1))
            rows.append((above, below, take(value, (1, 0)), take(above, (1, 0)), take(below, (1, 0))))
        return rows

    def keep(y, rows):
        for orb, values in enumerate(rows):
            for which, value in enumerate(values):
                ahead[which, y, orb] = value

    def apply(y, total):
        rows = {0: y, 1: lax.rem(y + 1, high), -1: lax.rem(y + high - 1, high)}
        coming = lax.rem(y + 2, high)
        spread_rows = spread(coming)

        def factor(row, i, j, k):
            place = j % 2 * 8 + i * 2 + j // 2
            return coef[row, k, place : place + 1, :]

        here = [field[y, orb] for orb in range(orbitals)]
        result = [shift * value for value in here]
        for j in range(orbitals):
            for i in range(orbitals):
                result[i] = result[i] + factor(y, i, j, ONSITE) * here[j]
        for k, (first, second, third) in enumerate(half_offsets):
            for j in range(orbitals):
                if (first, third) == (0, 0):
                    value = field[rows[second], j]
                else:
                    value = ahead[directions.index((first, third)), rows[second], j]
                for i in range(orbitals):
                    result[i] = result[i] + factor(y, i, j, k) * value
        landing = {}
        for first, third in ((1, 1), (1, -1), (1, 0), (0, 1), (0, -1), (0, 0)):
            sums = [None] * orbitals
            for k, offset in enumerate(half_offsets):
                if (offset[0], offset[2]) != (first, third):
                    continue
                row = rows[-offset[1]]
                for j in range(orbitals):
                    value = field[row, j]
                    for i in range(orbitals):
                        term = factor(row, j, i, k) * value
                        sums[i] = term if sums[i] is None else sums[i] + term
            if third == 1:
                sums = [take(value, (0, -1)) for value in sums]
            elif third == -1:
                sums = [take(value, (0, 1)) for value in sums]
            landing[first] = [a + b for a, b in zip(landing[first], sums)] if first in landing else sums
        for i in range(orbitals):
            value = result[i] + landing[0][i] + take(landing[1][i], (-1, 0))
            image[y, i] = value
            total = total + value * here[i]
        keep(coming, spread_rows)
        return total

    for iteration in range(ITERS):
        for y in (high - 1, 0, 1):
            keep(y, spread(y))
        product = jnp.sum(lax.fori_loop(0, high, apply, zero, unroll=4), axis=1, keepdims=True)
        alpha = norm_now / product

        def advance(y, total):
            for orb in range(orbitals):
                move = alpha * field[y, orb]
                answer[y, orb] = move if iteration == 0 else answer[y, orb] + move
                value = residual[y, orb] - alpha * image[y, orb]
                residual[y, orb] = value
                total = total + value * value
            return total

        total = lax.fori_loop(0, high, advance, zero, unroll=4)
        if iteration + 1 < ITERS:
            norm_next = jnp.sum(total, axis=1, keepdims=True)
            ratio = norm_next / norm_now

            def turn(y, carry):
                for orb in range(orbitals):
                    field[y, orb] = residual[y, orb] + ratio * field[y, orb]
                return carry

            lax.fori_loop(0, high, turn, 0, unroll=4)
            norm_now = norm_next

    for which, source in enumerate((answer, residual)):
        for gy in range(count_y):
            for tile in range(tiles):
                for half in range(ly // 2):
                    lanes = slice(tile * LANES, (tile + 1) * LANES)
                    parts = [source[gy * ly + half * 2 + g % 2, g // 2, :, lanes] for g in range(PARTS)]
                    for p, value in enumerate(turn_groups(parts, lane, strides)):
                        out_ref[device_of(tile * PARTS + p, gy), which, :, half * LANES : (half + 1) * LANES] = value


def block_kernel(bonds_hbm, open_hbm, onsite_hbm, levels_hbm, out_ref, rows, bonds_ref, open_ref, onsite_ref, levels_ref, sems):
    copies = [
        pltpu.make_async_copy(source, target, sems.at[n])
        for n, (source, target) in enumerate(
            ((bonds_hbm, bonds_ref), (open_hbm, open_ref), (onsite_hbm, onsite_ref), (levels_hbm, levels_ref))
        )
    ]
    for copy in copies:
        copy.start()
    orbitals, lx, ly, lz = levels_ref.shape
    bonds = bonds_ref.shape[-1]
    rows[...] = jnp.zeros_like(rows)
    for copy in copies:
        copy.wait()
    eye = (
        lax.broadcasted_iota(jnp.int32, (lz, lz), 0) == lax.broadcasted_iota(jnp.int32, (lz, lz), 1)
    ).astype(jnp.float32)
    for i in range(orbitals):
        for j in range(orbitals):
            for x in range(lx):
                local = 0.5 * (onsite_ref[i, j, x] + onsite_ref[j, i, x])
                if i == j:
                    local = local + levels_ref[i, x]
                for y in range(ly):
                    row = ((((i * orbitals + j) * (ly // 2) + y // 2) * lx + x) * 2 + y % 2) * lz
                    mask = open_ref[x * ly + y].astype(jnp.float32)
                    rows[row : row + lz, :bonds] = bonds_ref[((i * orbitals + j) * lx + x) * ly + y] * mask
                    rows[row : row + lz, bonds : bonds + lz] = eye * local[y : y + 1, :]
    turned = jnp.transpose(rows[...])
    last = jnp.sum(turned[bonds : bonds + lz], axis=0, keepdims=True)
    for part in range(turned.shape[1] // LANES):
        lanes = slice(part * LANES, (part + 1) * LANES)
        step = turned.shape[1] // LANES
        out_ref[pl.ds(part, 8, stride=step), :] = turned[:8, lanes]
        out_ref[pl.ds(8 * step + part, bonds - 8, stride=step), :] = turned[8:bonds, lanes]
        out_ref[bonds * step + part : bonds * step + part + 1, :] = last[:, lanes]


def pack_kernel(field_ref, out_ref, rows):
    lx, ly, lz, orbitals, _ = field_ref.shape
    for x in range(lx):
        for y in range(ly):
            for z in range(lz):
                base = ((y // 2 * orbitals * lx + x) * 2 + y % 2) * lz + z
                for tile in range(rows.shape[0]):
                    lanes = slice(tile * LANES, (tile + 1) * LANES)
                    rows[tile, pl.ds(base, orbitals, stride=2 * lx * lz), :] = field_ref[x, y, z, :, lanes]
    for tile in range(rows.shape[0]):
        out_ref[tile * LANES : (tile + 1) * LANES, :] = jnp.transpose(rows[tile])


def unpack_kernel(back_ref, answer_ref, residual_ref, rows):
    lx, ly, lz, orbitals, columns = answer_ref.shape
    for which, out_ref in enumerate((answer_ref, residual_ref)):
        turned = jnp.transpose(back_ref[:, which].reshape(columns, -1))
        for tile in range(rows.shape[1]):
            rows[which, tile] = turned[:, tile * LANES : (tile + 1) * LANES]
        for x in range(lx):
            for y in range(ly):
                for z in range(lz):
                    base = ((y // 2 * orbitals * lx + x) * 2 + y % 2) * lz + z
                    for tile in range(rows.shape[1]):
                        lanes = slice(tile * LANES, (tile + 1) * LANES)
                        out_ref[x, y, z, :, lanes] = rows[which, tile, pl.ds(base, orbitals, stride=2 * lx * lz), :]


def per_device(right_side, bond_blocks, bond_open, onsite_blocks, orbital_levels, column_shift):
    lx, ly, lz, orbitals, columns = right_side.shape
    count_x, count_y, count_z = (lax.axis_size(axis) for axis in ALL)
    devices = count_x * count_y * count_z
    own_columns = columns // devices
    padded = -(-own_columns // 8) * 8
    width = count_x * count_z * lx * lz
    high = count_y * ly
    assert (lx, ly, lz, orbitals) == (4, 4, 4, 4) and columns % devices == 0
    assert count_x % 2 == 0 and count_y % 2 == 0 and count_x * count_z % PARTS == 0

    atoms = lx * ly * lz
    bonds = bond_blocks.shape[0]
    vmem = pl.BlockSpec(memory_space=pltpu.VMEM)
    inputs = (
        jnp.transpose(bond_blocks, (1, 2, 3, 4, 5, 0)).reshape(-1, lz, bonds),
        jnp.transpose(bond_open, (1, 2, 3, 0)).reshape(-1, lz, bonds),
        onsite_blocks,
        orbital_levels,
    )
    block = pl.pallas_call(
        block_kernel,
        out_shape=jax.ShapeDtypeStruct(((bonds + 1) * orbitals * orbitals * atoms // LANES, LANES), jnp.float32),
        in_specs=[pl.BlockSpec(memory_space=pltpu.HBM)] * 4,
        out_specs=vmem,
        scratch_shapes=[pltpu.VMEM((orbitals * orbitals * atoms, LANES), jnp.float32)]
        + [pltpu.VMEM(value.shape, value.dtype) for value in inputs]
        + [pltpu.SemaphoreType.DMA((4,))],
        compiler_params=pltpu.CompilerParams(vmem_limit_bytes=60 * 1024 * 1024),
        name="block",
    )(*inputs)
    own, other = gather_blocks(block)

    packed = pl.pallas_call(
        pack_kernel,
        out_shape=jax.ShapeDtypeStruct((columns, orbitals * atoms), jnp.float32),
        in_specs=[vmem],
        out_specs=vmem,
        scratch_shapes=[pltpu.VMEM((columns // LANES, orbitals * atoms, LANES), jnp.float32)],
        compiler_params=pltpu.CompilerParams(vmem_limit_bytes=3 * 1024 * 1024),
        name="pack",
    )(right_side)
    packed = packed.reshape(devices, own_columns, orbitals * atoms)
    received = lax.all_to_all(packed, ALL, 0, 0, tiled=True)
    index = (lax.axis_index("gx") * count_y + lax.axis_index("gy")) * count_z + lax.axis_index("gz")
    shift = lax.dynamic_slice_in_dim(column_shift, index * own_columns, own_columns)
    if padded != own_columns:
        received = jnp.pad(received, ((0, 0), (0, padded - own_columns), (0, 0)))
        shift = jnp.pad(shift, (0, padded - own_columns))
    shift = jnp.broadcast_to(shift[:, None], (padded, width))

    sizes = (count_x, count_y, count_z, lx, ly, lz, orbitals)
    masks = [lanes for plan in all_plans(sizes).values() for _, lanes in plan[1:]]
    masks = jnp.asarray(np.stack(masks).astype(np.int32))
    state = pltpu.VMEM((high, orbitals, padded, width), jnp.float32)
    out = pl.pallas_call(
        functools.partial(cg_kernel, sizes),
        out_shape=jax.ShapeDtypeStruct((devices, 2, padded, orbitals * lx * ly * lz), jnp.float32),
        in_specs=[vmem] * 5,
        out_specs=vmem,
        scratch_shapes=[
            pltpu.VMEM((high, ONSITE + 1, orbitals * orbitals, width), jnp.float32),
            state,
            state,
            state,
            state,
            pltpu.VMEM((5, high, orbitals, padded, width), jnp.float32),
        ],
        compiler_params=pltpu.CompilerParams(vmem_limit_bytes=(8 + 24 * width // 512) * 1024 * 1024 * 2),
        name="cg",
    )(received, own, other, shift, masks)
    if padded != own_columns:
        out = out[:, :, :own_columns]
    back = lax.all_to_all(out, ALL, 0, 0, tiled=True)
    shape = jax.ShapeDtypeStruct(right_side.shape, jnp.float32)
    return tuple(
        pl.pallas_call(
            unpack_kernel,
            out_shape=(shape, shape),
            in_specs=[vmem],
            out_specs=(vmem, vmem),
            scratch_shapes=[pltpu.VMEM((2, columns // LANES, orbitals * atoms, LANES), jnp.float32)],
            compiler_params=pltpu.CompilerParams(vmem_limit_bytes=6 * 1024 * 1024),
            name="unpack",
        )(back)
    )


def solution(mesh):
    placed = (
        P("gx", "gy", "gz", None, None),
        P(None, None, None, "gx", "gy", "gz"),
        P(None, "gx", "gy", "gz"),
        P(None, None, "gx", "gy", "gz"),
        P(None, "gx", "gy", "gz"),
        P(),
    )
    return jax.shard_map(
        per_device,
        mesh=mesh,
        in_specs=placed,
        out_specs=(P("gx", "gy", "gz", None, None), P("gx", "gy", "gz", None, None)),
        check_vma=False,
    )
```
